32 devices in a mesh: sample: 4 (over z), seq: 2 (over core), tensor: 4 (over y, x).
Axes of the slice: x: 2, y: 2, z: 4, core: 2. Of those that a mesh axis runs over, the one named last changes fastest.
Arguments:
- hidden: bfloat16 [4, 256, 4096], P('sample', 'seq'), may hold values from -512 to 512
- weight: bfloat16 [4096, 81920], P(None, ('sample', 'tensor')), may hold values from -1 to 1
- targets: int32 [4, 256], P('sample', 'seq'), may hold values from 0 to 81919
- old_logprob: float32 [4, 256], P('sample', 'seq'), may hold values from -13.65 to -10.65
- lengths: int32 [4], replicated, may hold values from 1 to 256, 640 in all
- group_ids: int32 [4], replicated, may hold values from 0 to 1, as said below
- rewards: int32 [4], P('sample'), may hold values from 0 to 2000
Outputs:
- new_logprob: float32 [4, 256], P('sample', 'seq')
- advantage: float32 [4], P('sample')
- completion_term: float32 [4], P('sample')
- loss: float32 [], replicated
The draws below stay inside these ranges and needn't reach their ends.
Inputs may be any that keep to these rules, and one draw needn't show every extreme that they name: The lengths sum to 640 and one equals 256. `group_ids`: each prompt id names exactly 2 completions.
All inputs are finite; a program needn't handle non-finite values.
Results may differ from the reference program's by a relative error of at most 0.0003.
Values may be sent and summed in bfloat16 or wider, within the bound.
A program may use at most 128 MiB of HBM per device.

```python
import math
import jax
import jax.numpy as jnp
import numpy as np
from jax import lax

D = 4096
VOCAB = 81920
LEN = 256
GROUP = 2
COMPLETIONS = 4


def weight_column(base, column):
    direction = jax.random.truncated_normal(jax.random.fold_in(base, column), -4.0, 4.0, (D,), jnp.float32) / math.sqrt(D)
    scale_key = jax.random.fold_in(jax.random.fold_in(base, 104729), column)
    column_scale = jnp.exp(jax.random.uniform(scale_key, (), jnp.float32, math.log(0.5), math.log(2.0)))
    return direction * column_scale


def draw_weight(key, part):
    base = jax.random.fold_in(key, 7)
    columns = jax.vmap(lambda column: weight_column(base, column))(jnp.arange(VOCAB, dtype=jnp.int32))
    return columns.astype(jnp.bfloat16).T


def draw_group_ids(key, part):
    shuffled = jax.random.permutation(jax.random.fold_in(key, 13), jnp.arange(COMPLETIONS, dtype=jnp.int32))
    return (shuffled // GROUP).astype(jnp.int32)


def draw_hidden(key, part):
    base = jax.random.fold_in(key, 11)
    values = jax.random.truncated_normal(jax.random.fold_in(base, 5), -6.0, 6.0, (COMPLETIONS, LEN, D), jnp.float32)
    return values.astype(jnp.bfloat16)


def place_ends(values, stream_key, smallest, high):
    longest = values.shape.index(max(values.shape))
    spots = []
    for shift in (0, 1):
        where = [jax.random.randint(jax.random.fold_in(stream_key, axis), (), 0, length) for axis, length in enumerate(values.shape)]
        where[longest] = (where[longest] + shift) % values.shape[longest]
        spots.append(tuple(where))
    return values.at[spots[0]].set(smallest).at[spots[1]].set(high)


def block_scale(own_key, extent, shards, smallest, top_value):
    level = 1.0
    for position, blocks in shards:
        draws = jax.random.uniform(jax.random.fold_in(jax.random.fold_in(own_key, 6), position), (blocks,), jnp.float32, smallest / len(shards), top_value / len(shards))
        level = level * jnp.repeat(jnp.exp(draws), extent[position] // blocks).reshape((-1,) + (1,) * (len(extent) - 1 - position))
    return level


def ranked_wide(own_key, shape, count, slope):
    loads = [min(1 << octave, count + 1 - (1 << octave)) * (1 << 20) // math.isqrt((1 << octave) ** slope) + 1 for octave in range((count + 1).bit_length()) if 1 << octave <= count]
    width = 1 + sum(loads) // (1 << 30)
    table = np.cumsum(np.array([max(1, weight // width) for weight in loads]))
    ticket = jax.random.randint(jax.random.fold_in(own_key, 1), shape, 0, int(table[len(loads) - 1]))
    start = jnp.left_shift(1, jnp.searchsorted(jnp.asarray(table, jnp.int32), ticket, side="right").astype(jnp.int32))
    grade = start - 1 + jax.random.randint(jax.random.fold_in(own_key, 4), shape, 0, 1 << 30) % jnp.minimum(start, count + 1 - start)
    return jax.random.permutation(jax.random.fold_in(own_key, 2), count)[grade].astype(jnp.int32)


def split_up(count, total, most, slope):
    portions = [(1 << 20) // math.isqrt(grade ** slope) + 1 for grade in range(2, count + 1)]
    surplus, counts = total - most - (count - 1), [1] * (count - 1)
    while surplus > 0:
        free = [i for i in range(count - 1) if counts[i] < most]
        mass, remaining = sum([portions[i] for i in free]), surplus
        for i in free:
            extra = min(most - counts[i], max(1, remaining * portions[i] // mass), surplus)
            counts[i] = counts[i] + extra
            surplus = surplus - extra
    return np.array([most] + counts)


def ragged(own_key, amount, total, reach, skew):
    if amount == 2:
        one = jax.random.randint(own_key, (), max(1, total - reach), min(reach, total - 1) + 1)
        return jnp.stack([one, total - one])
    sizes = jnp.asarray(split_up(amount, total, reach, skew), jnp.int32)
    pairs = (amount - 1) // 2
    source_of, taker = sizes[1:1 + 2 * pairs:2], sizes[2:2 + 2 * pairs:2]
    slack = jnp.minimum(source_of - 1, reach - taker)
    moved = jax.random.randint(jax.random.fold_in(own_key, 1), (pairs,), 0, 1 << 20) % (slack + 1)
    sizes = sizes.at[1:1 + 2 * pairs:2].set(source_of - moved).at[2:2 + 2 * pairs:2].set(taker + moved)
    return sizes[jax.random.permutation(jax.random.fold_in(own_key, 2), amount)]


def setup_inputs(seed: int = 0) -> dict:
    seeds = jax.random.split(jax.random.key(seed), 8)
    hidden = draw_hidden(jax.random.fold_in(seeds[7], 71), 0)
    weight = draw_weight(jax.random.fold_in(seeds[7], 71), 0)
    targets = place_ends(ranked_wide(seeds[2], (COMPLETIONS, LEN), VOCAB, 2), jax.random.fold_in(seeds[2], 3), 0, VOCAB - 1).astype(jnp.int32)
    old_logprob = jnp.clip(-13.65 + 3.0 * jax.random.uniform(seeds[3], (COMPLETIONS, LEN), jnp.float32) ** block_scale(seeds[3], (COMPLETIONS, LEN), ((0, 4), (1, 2)), -0.2, 0.2), -13.65, -10.65)
    lengths = ragged(seeds[4], COMPLETIONS, COMPLETIONS * LEN * 5 // 8, LEN, 2).astype(jnp.int32)
    group_ids = draw_group_ids(jax.random.fold_in(seeds[7], 71), 0)
    rewards = place_ends(jax.random.randint(seeds[6], (COMPLETIONS,), 0, 2001), jax.random.fold_in(seeds[6], 1), 0, 2000).astype(jnp.int32)
    return {"hidden": hidden, "weight": weight, "targets": targets, "old_logprob": old_logprob, "lengths": lengths, "group_ids": group_ids, "rewards": rewards}


CLIP_LOW = 0.8
CLIP_HIGH = 1.28
VAR_FLOOR = 0.25
REWARD_SCALE = 1000.0

def token_logprobs(hidden, weight, targets):

    def single(inputs):
        row_block, token_ids = inputs
        logits = jnp.dot(row_block, weight, preferred_element_type=jnp.float32)
        highest = lax.optimization_barrier(jnp.max(logits, axis=1))
        log_norm = highest + jnp.log(lax.optimization_barrier(jnp.sum(jnp.exp(logits - highest[:, None]), axis=1)))
        picked = jnp.take_along_axis(logits, token_ids[:, None].astype(jnp.int32), axis=1)[:, 0]
        return picked - log_norm
    return lax.map(single, (hidden, targets))

def reference(hidden, weight, targets, old_logprob, lengths, group_ids, rewards):
    raw_logprob = token_logprobs(hidden, weight, targets)
    positions = lax.broadcasted_iota(jnp.int32, raw_logprob.shape, 1)
    usable = positions < lengths[:, None]
    new_logprob = jnp.where(usable, raw_logprob, jnp.float32(0.0))
    reward = rewards.astype(jnp.float32) / REWARD_SCALE
    groups = COMPLETIONS // GROUP
    member = (group_ids[:, None] == jnp.arange(groups, dtype=jnp.int32)[None, :]).astype(jnp.float32)
    group_mean = lax.optimization_barrier(jnp.sum(member * reward[:, None], axis=0)) / GROUP
    group_square = lax.optimization_barrier(jnp.sum(member * (reward * reward)[:, None], axis=0)) / GROUP
    group_scale = jnp.sqrt(jnp.maximum(group_square - group_mean * group_mean, VAR_FLOOR))
    advantage = (reward - group_mean[group_ids]) / group_scale[group_ids]
    ratios = jnp.exp(new_logprob - old_logprob)
    clipped = jnp.clip(ratios, CLIP_LOW, CLIP_HIGH)
    objective = jnp.where(usable, jnp.minimum(ratios * advantage[:, None], clipped * advantage[:, None]), jnp.float32(0.0))
    completion_term = lax.optimization_barrier(jnp.sum(objective, axis=1)) / lengths.astype(jnp.float32)
    loss = -jnp.sum(completion_term) / COMPLETIONS
    return (new_logprob, advantage, completion_term, loss)
```

```python
import functools

import jax
import jax.numpy as jnp
from jax import lax
from jax.experimental import pallas as pl
from jax.experimental.pallas import tpu as pltpu
from jax.sharding import PartitionSpec as P

GROUP = 2


CLIP_LOW = 0.8
CLIP_HIGH = 1.28
VAR_FLOOR = 0.25
REWARD_SCALE = 1000.0
LANES = 128
MESH = pl.DeviceIdType.MESH
Z, X, Y, DX, DY, CZ, CX, CY, CD = range(9)


def not_negative(value, bound):
    return lax.div(value + bound, bound)


def merge(stats):
    highest = functools.reduce(jnp.maximum, [s[0:1] for s in stats])
    summed = sum(s[1:2] * jnp.exp(s[0:1] - highest) for s in stats)
    picked = sum(s[2:3] for s in stats)
    return highest, summed, picked


def store_stats(ref, highest, summed, picked):
    ref[0:1, :] = highest
    ref[1:2, :] = summed
    ref[2:3, :] = picked


def kernel(
    sizes,
    hidden_ref,
    weight_ref,
    aux_ref,
    length_ref,
    same_ref,
    out_ref,
    rows,
    w,
    aux,
    run,
    stat,
    arrived_a,
    joined,
    arrived_b,
    term,
    arrived_c,
    send,
    recv,
    own_sem,
    w_sem,
    aux_send,
    aux_recv,
    a_send,
    a_recv,
    b_send,
    b_recv,
    c_send,
    c_recv,
):
    samples, tensors, half, tiles, tile = sizes
    s = lax.axis_index("sample")
    c = lax.axis_index("seq")
    t = lax.axis_index("tensor")
    other = 1 - c
    x_near = t + 1 - 2 * lax.rem(t, 2)
    y_near = t + 2 - 4 * lax.div(t, 2)
    unit = half // tensors
    part = unit // 2
    local = pltpu.make_async_copy(
        hidden_ref, rows.at[s, pl.ds(pl.multiple_of(c * half, half), half)], own_sem.at[0]
    )
    local.start()
    width = tiles * tile

    def weight_copy(i):
        first = pl.multiple_of(c * width + i * tile, LANES)
        return pltpu.make_async_copy(weight_ref.at[:, pl.ds(first, tile)], w.at[i], w_sem.at[i])

    for i in range(tiles):
        weight_copy(i).start()

    def at_column(k):
        return {"sample": lax.rem(s + k // 2, samples), "seq": lax.rem(c + k % 2, 2)}

    def in_plane(k):
        return {"seq": lax.rem(c + k % 2, 2), "tensor": lax.rem(t + k // 2, tensors)}

    barrier = pltpu.get_barrier_semaphore()
    for k in range(1, 2 * samples):
        pl.semaphore_signal(barrier, inc=1, device_id=at_column(k), device_id_type=MESH)
    for k in range(2, 2 * tensors):
        pl.semaphore_signal(barrier, inc=1, device_id=in_plane(k), device_id_type=MESH)
    pl.semaphore_wait(barrier, 2 * samples - 1 + 2 * tensors - 2)

    def remote(src, dst, send_sem, recv_sem, device):
        return pltpu.make_async_remote_copy(
            src_ref=src,
            dst_ref=dst,
            send_sem=send_sem,
            recv_sem=recv_sem,
            device_id=device,
            device_id_type=MESH,
        )

    def piece(plane, core, owner, shift, count):
        return rows.at[plane, pl.ds(pl.multiple_of(core * half + owner * unit + shift, 16), count)]

    def moved(kind, plane, owner, shift, count, device):
        ref = piece(plane, c, owner, shift, count)
        return remote(ref, ref, send.at[kind, plane], recv.at[kind, plane], device)

    def awaited(kind, plane, core, owner, shift, count):
        ref = piece(plane, core, owner, shift, count)
        remote(ref, ref, send.at[kind, plane], recv.at[kind, plane], {"seq": other}).wait_recv()

    local.wait()
    own_unit = piece(s, c, t, 0, unit)
    own_rows = rows.at[s, pl.ds(pl.multiple_of(c * half, half), half)]
    to_right = remote(own_unit, own_unit, own_sem.at[1], recv.at[Z, s], {"sample": lax.rem(s + 1, samples)})
    to_left = remote(
        own_unit, own_unit, own_sem.at[2], recv.at[Z, s], {"sample": lax.rem(s + samples - 1, samples)}
    )
    to_core = remote(own_rows, own_rows, own_sem.at[3], recv.at[CZ, s], {"seq": other})
    pl.when(s < samples - 1)(to_right.start)
    pl.when(s > 0)(to_left.start)

    def aux_copy(k):
        return remote(
            aux_ref, aux.at[2 * s + c], aux_send.at[k], aux_recv.at[2 * s + c], at_column(k)
        )

    for k in range(1, 2 * samples):
        aux_copy(k).start()
    to_core.start()
    aux[2 * s + c] = aux_ref[...]
    for k in range(1, 2 * samples):
        source = 2 * lax.rem(s + k // 2, samples) + lax.rem(c + k % 2, 2)
        remote(aux_ref, aux.at[source], aux_send.at[k], aux_recv.at[source], {"seq": other}).wait_recv()

    pairs = jnp.minimum(s, samples - 1 - s)
    rightward = not_negative(samples - 1 - 2 * s, 2 * samples)

    def plane_of(j):
        if j == 0:
            return s
        single = not_negative(j - 2 * pairs - 1, 2 * samples)
        paired = s + (j + 1) // 2 * (1 if j % 2 else -1)
        alone = s + (2 * rightward - 1) * (j - pairs)
        return paired + single * (alone - paired)

    planes = [plane_of(j) for j in range(samples)]

    def onward(p):
        from_left = not_negative(s - p, 2 * samples)
        nxt = s + 2 * from_left - 1
        inside = (nxt >= 0) & (nxt < samples)
        copy = moved(Z, p, t, 0, unit, {"sample": lax.rem(nxt + samples, samples)})
        return inside, copy

    def sends(j):
        p = planes[j]
        return {
            X: lambda: moved(X, p, t, 0, unit, {"tensor": x_near}),
            Y: lambda: moved(Y, p, t, 0, unit, {"tensor": y_near}),
            CZ: lambda: moved(CZ, p, t, 0, unit, {"seq": other}),
            DY: lambda: moved(DY, p, x_near, 0, part, {"tensor": y_near}),
            CX: lambda: moved(CX, p, x_near, 0, unit, {"seq": other}),
            DX: lambda: moved(DX, p, y_near, part, part, {"tensor": x_near}),
            CY: lambda: moved(CY, p, y_near, 0, unit, {"seq": other}),
            CD: lambda: moved(CD, p, tensors - 1 - t, 0, unit, {"seq": other}),
        }

    def event_z(j):
        p = planes[j]
        awaited(Z, p, c, t, 0, unit)
        inside, copy = onward(p)
        pl.when(inside)(copy.start)
        out = sends(j)
        out[X]().start()
        out[Y]().start()
        out[CZ]().start()

    def event_xy(j):
        p = planes[j]
        out = sends(j)
        awaited(X, p, c, x_near, 0, unit)
        out[DY]().start()
        out[CX]().start()
        awaited(Y, p, c, y_near, 0, unit)
        out[DX]().start()
        out[CY]().start()

    def event_d(j):
        p = planes[j]
        far = tensors - 1 - t
        awaited(DY, p, c, far, 0, part)
        awaited(DX, p, c, far, part, part)
        sends(j)[CD]().start()

    def from_core(j):
        p = planes[j]
        if j == 0:
            block = rows.at[p, pl.ds(pl.multiple_of(other * half, half), half)]
            remote(block, block, own_sem.at[3], recv.at[CZ, p], {"seq": other}).wait_recv()
            return
        awaited(CZ, p, other, t, 0, unit)
        awaited(CX, p, other, x_near, 0, unit)
        awaited(CY, p, other, y_near, 0, unit)
        awaited(CD, p, other, tensors - 1 - t, 0, unit)

    slice_start = ((s * tensors + t) * 2 + c) * width

    def begin(j):
        from_core(j)
        p = planes[j]
        run[0] = jnp.full((2 * half, LANES), -jnp.inf, jnp.float32)
        run[1] = jnp.zeros((2 * half, LANES), jnp.float32)
        run[2] = jnp.zeros((2 * half, LANES), jnp.float32)
        for h in range(2):
            ids = jnp.broadcast_to(aux[2 * p + h][2:3, :], (LANES, half))
            run[3, h * half : (h + 1) * half, :] = ids.T

    def compute(j, first, last):
        p = planes[j]

        def step(i, carry):
            if j == 0:
                weight_copy(i).wait()
            logits = jnp.dot(rows[p], w[i], preferred_element_type=jnp.float32)
            chunks = [logits[:, k : k + LANES] for k in range(0, tile, LANES)]
            before = run[0]
            highest = functools.reduce(jnp.maximum, chunks, before)
            run[0] = highest
            run[1] = run[1] * jnp.exp(before - highest) + sum(jnp.exp(x - highest) for x in chunks)
            lane = lax.broadcasted_iota(jnp.int32, (2 * half, LANES), 1)
            wanted = run[3].astype(jnp.int32) - (slice_start + i * tile)
            run[2] += sum(
                jnp.where(lane + k * LANES == wanted, x, jnp.float32(0.0)) for k, x in enumerate(chunks)
            )
            return carry

        lax.fori_loop(first, last, step, 0)

    def finish(j):
        p = planes[j]
        highest = run[0].T
        top = jnp.max(highest, axis=0, keepdims=True)
        summed = jnp.sum(run[1].T * jnp.exp(highest - top), axis=0, keepdims=True)
        picked = jnp.sum(run[2].T, axis=0, keepdims=True)
        store_stats(stat.at[p], top, summed, picked)
        if j:
            stage_a(j).start()

    def stage_a(j):
        p = planes[j]
        return remote(stat.at[p], arrived_a.at[s], a_send.at[p], a_recv.at[s], {"sample": p})

    begin(0)
    compute(0, 0, tiles)
    finish(0)
    event_z(1)
    cut = tiles // 2
    for j in range(1, samples):
        if j + 1 < samples:
            event_z(j + 1)
        if j >= 2:
            begin(j - 1)
            compute(j - 1, 0, cut)
        event_xy(j)
        if j >= 2:
            compute(j - 1, cut, tiles)
            finish(j - 1)
        event_d(j)
    begin(samples - 1)
    compute(samples - 1, 0, tiles)
    finish(samples - 1)

    group_sum = jnp.zeros((1, LANES), jnp.float32)
    group_square = jnp.zeros((1, LANES), jnp.float32)
    for p in range(samples):
        reward = aux[2 * p][1:2, :]
        group_sum += same_ref[p : p + 1, :] * reward
        group_square += same_ref[p : p + 1, :] * (reward * reward)
    group_mean = group_sum / GROUP
    group_scale = jnp.sqrt(jnp.maximum(group_square / GROUP - group_mean * group_mean, VAR_FLOOR))
    advantage = (aux_ref[1:2, :] - group_mean) / group_scale

    collected = [stat[s]]
    for k in range(1, samples):
        source = lax.rem(s + k, samples)
        remote(stat.at[s], arrived_a.at[source], a_send.at[source], a_recv.at[source], {"sample": source}).wait_recv()
        collected.append(arrived_a[source])
    store_stats(joined, *merge(collected))

    def stage_b(k):
        here = 2 * t + c
        return remote(joined, arrived_b.at[here], b_send.at[k], b_recv.at[here], in_plane(k))

    for k in range(1, 2 * tensors):
        stage_b(k).start()
    collected = [joined[...]]
    for k in range(1, 2 * tensors):
        source = 2 * lax.rem(t + k // 2, tensors) + lax.rem(c + k % 2, 2)
        remote(joined, arrived_b.at[source], b_send.at[k], b_recv.at[source], {"seq": other}).wait_recv()
        collected.append(arrived_b[source])
    highest, summed, picked = merge(collected)
    logprob = picked - (highest + jnp.log(summed))
    total = jnp.zeros((1, 1), jnp.float32)
    halves = []
    length = length_ref[0:1, :]
    for h in range(2):
        position = h * half + lax.broadcasted_iota(jnp.int32, (1, half), 1)
        usable = position.astype(jnp.float32) < length
        new = jnp.where(usable, logprob[:, h * half : (h + 1) * half], jnp.float32(0.0))
        halves.append(new)
        ratios = jnp.exp(new - aux[2 * s + h][0:1, :])
        clipped = jnp.clip(ratios, CLIP_LOW, CLIP_HIGH)
        objective = jnp.where(
            usable, jnp.minimum(ratios * advantage, clipped * advantage), jnp.float32(0.0)
        )
        total += jnp.sum(objective, axis=1, keepdims=True)
    own_term = jnp.broadcast_to(total, (1, LANES)) / length
    term[...] = jnp.broadcast_to(own_term, term.shape)

    def stage_c(k):
        return remote(
            term, arrived_c.at[s], c_send.at[k], c_recv.at[s], {"sample": lax.rem(s + k, samples)}
        )

    for k in range(1, samples):
        stage_c(k).start()
    mine = c.astype(jnp.float32)
    out_ref[0:1, :] = halves[0] * (1.0 - mine) + halves[1] * mine
    out_ref[1:2, :] = advantage
    out_ref[2:3, :] = own_term
    loss = own_term
    for k in range(1, samples):
        source = lax.rem(s + k, samples)
        remote(term, arrived_c.at[source], c_send.at[k], c_recv.at[source], {"seq": other}).wait_recv()
    arrived_c[s] = term[...]
    loss = sum(arrived_c[p][0:1, :] for p in range(samples))
    out_ref[3:4, :] = -loss / samples
    out_ref[4:8, :] = jnp.zeros((4, LANES), jnp.float32)

    pl.when(s < samples - 1)(to_right.wait_send)
    pl.when(s > 0)(to_left.wait_send)
    to_core.wait_send()
    for k in range(1, 2 * samples):
        aux_copy(k).wait_send()
    for j in range(1, samples):
        inside, copy = onward(planes[j])
        pl.when(inside)(copy.wait_send)
        for copy in sends(j).values():
            copy().wait_send()
        stage_a(j).wait_send()
        stage_c(j).wait_send()
    for k in range(1, 2 * tensors):
        stage_b(k).wait_send()


def per_device(hidden, weight, targets, old_logprob, lengths, group_ids, rewards):
    _, half, model_width = hidden.shape
    samples = lax.axis_size("sample")
    tensors = lax.axis_size("tensor")
    width = weight.shape[1] // 2
    tile = max(n for n in range(LANES, 513, LANES) if width % n == 0)
    tiles = width // tile
    s = lax.axis_index("sample")
    reward = rewards.astype(jnp.float32) / REWARD_SCALE
    aux = jnp.concatenate(
        [
            old_logprob,
            jnp.broadcast_to(reward[:, None], (1, half)),
            targets.astype(jnp.float32),
            jnp.zeros((5, half), jnp.float32),
        ]
    )
    own_length = lax.dynamic_slice_in_dim(lengths, s, 1).astype(jnp.float32)
    own_group = lax.dynamic_slice_in_dim(group_ids, s, 1)
    length = jnp.broadcast_to(own_length[:, None], (8, LANES))
    same = jnp.broadcast_to((group_ids == own_group).astype(jnp.float32)[:, None], (samples, LANES))
    f32 = jnp.float32
    dma = pltpu.SemaphoreType.DMA
    vmem = pl.BlockSpec(memory_space=pltpu.VMEM)
    out = pl.pallas_call(
        functools.partial(kernel, (samples, tensors, half, tiles, tile)),
        out_shape=jax.ShapeDtypeStruct((8, LANES), f32),
        in_specs=[
            pl.BlockSpec(memory_space=pltpu.HBM),
            pl.BlockSpec(memory_space=pltpu.HBM),
            vmem,
            vmem,
            vmem,
        ],
        out_specs=vmem,
        scratch_shapes=[
            pltpu.VMEM((samples, 2 * half, model_width), jnp.bfloat16),
            pltpu.VMEM((tiles, model_width, tile), jnp.bfloat16),
            pltpu.VMEM((2 * samples, 8, half), f32),
            pltpu.VMEM((4, 2 * half, LANES), f32),
            pltpu.VMEM((samples, 8, 2 * half), f32),
            pltpu.VMEM((samples, 8, 2 * half), f32),
            pltpu.VMEM((8, 2 * half), f32),
            pltpu.VMEM((2 * tensors, 8, 2 * half), f32),
            pltpu.VMEM((8, LANES), f32),
            pltpu.VMEM((samples, 8, LANES), f32),
            dma((9, samples)),
            dma((9, samples)),
            dma((4,)),
            dma((tiles,)),
            dma((2 * samples,)),
            dma((2 * samples,)),
            dma((samples,)),
            dma((samples,)),
            dma((2 * tensors,)),
            dma((2 * tensors,)),
            dma((samples,)),
            dma((samples,)),
        ],
        compiler_params=pltpu.CompilerParams(
            collective_id=0, has_side_effects=True, vmem_limit_bytes=60 * 1024 * 1024
        ),
    )(hidden.reshape(half, model_width), weight, aux, length, same)
    return (out[0:1], out[1, 0:1], out[2, 0:1], out[3, 0])


def solution(mesh):
    placed = (
        P("sample", "seq", None),
        P(None, ("sample", "tensor")),
        P("sample", "seq"),
        P("sample", "seq"),
        P(),
        P(),
        P("sample"),
    )
    return jax.shard_map(
        per_device,
        mesh=mesh,
        in_specs=placed,
        out_specs=(P("sample", "seq"), P("sample"), P("sample"), P()),
        check_vma=False,
    )
```
